32 devices in a mesh: lat: 4 (over z), lon: 4 (over x, core), lev: 2 (over y).
Axes of the slice: x: 2, y: 2, z: 4, core: 2. Of those that a mesh axis runs over, the one named last changes fastest.
Arguments:
- field_now: float32 [16, 256, 128, 128], P('lat', 'lon', 'lev'), may hold values from 0.2 to 1.8
- earlier: float32 [16, 256, 128, 128], P('lat', 'lon', 'lev'), may hold values from 0.2 to 1.8
- speed_square: float32 [16, 256, 128, 128], P('lat', 'lon', 'lev'), may hold values from 0.05 to 0.3
Outputs:
- field_now_end: float32 [16, 256, 128, 128], P('lat', 'lon', 'lev')
The draws below stay inside these ranges and needn't reach their ends.
All inputs are finite; a program needn't handle non-finite values.
Results may differ from the reference program's by a relative error of at most 0.00002.
Values sent between devices are 32-bit elements; how exact they have to be, the bound alone decides.
A program may use at most 320 MiB of HBM per device.

```python
import jax
import jax.numpy as jnp
from jax import lax

GRID_J = 16
GRID_I = 256
GRID_K = 128
MEMBERS = 128
STEPS = 4


def block_levels(stream_key, shape, cuts, least, largest):
    def one(axis_at, blocks):
        draws = jax.random.uniform(jax.random.fold_in(jax.random.fold_in(stream_key, 6), axis_at), (blocks,), jnp.float32, least / len(cuts), largest / len(cuts))
        return jnp.repeat(jnp.exp(draws), shape[axis_at] // blocks).reshape((-1,) + (1,) * (len(shape) - axis_at - 1))

    gain = one(*cuts[0])
    for cut in cuts[1:]:
        gain = gain * one(*cut)
    return gain


def setup_inputs(seed: int = 0) -> dict:
    arg_keys = jax.random.split(jax.random.key(seed), 4)
    field_now = jnp.clip(0.2 + 1.5999999 * jax.random.uniform(arg_keys[0], (GRID_J, GRID_I, GRID_K, MEMBERS), jnp.float32) ** block_levels(arg_keys[0], (GRID_J, GRID_I, GRID_K, MEMBERS), ((0, 4), (1, 4), (2, 2)), -0.2, 0.2), 0.2, 1.8)
    earlier = jnp.clip(0.2 + 1.5999999 * jax.random.uniform(arg_keys[1], (GRID_J, GRID_I, GRID_K, MEMBERS), jnp.float32) ** block_levels(arg_keys[1], (GRID_J, GRID_I, GRID_K, MEMBERS), ((0, 4), (1, 4), (2, 2)), -0.2, 0.2), 0.2, 1.8)
    speed_square = jnp.clip(0.05 + 0.25 * jax.random.uniform(arg_keys[2], (GRID_J, GRID_I, GRID_K, MEMBERS), jnp.float32) ** block_levels(arg_keys[2], (GRID_J, GRID_I, GRID_K, MEMBERS), ((0, 4), (1, 4), (2, 2)), -0.2, 0.2), 0.05, 0.3)
    return {"field_now": field_now, "earlier": earlier, "speed_square": speed_square}


def without_rim(values, dims):
    for dim in dims:
        values = lax.slice_in_dim(values, 1, values.shape[dim] - 1, axis=dim)
    return values


def shifted_cells(values, dim, start, dims):
    others = [other for other in dims if other != dim]
    values = without_rim(values, others)
    return lax.slice_in_dim(values, start, start + values.shape[dim] - 2, axis=dim)


def march_step(padded, before, speed_square):
    middle = without_rim(padded, (0, 1, 2))
    lower = [shifted_cells(padded, dim, 0, (0, 1, 2)) for dim in (0, 1, 2)]
    upper = [shifted_cells(padded, dim, 2, (0, 1, 2)) for dim in (0, 1, 2)]
    spread = lower[0] + upper[0] + lower[1] + upper[1] + lower[2] + upper[2] - 6.0 * middle
    return 2.0 * middle - before + speed_square * spread


def reference(field_now, earlier, speed_square):
    for step in range(STEPS):
        later = march_step(jnp.pad(field_now, ((1, 1), (1, 1), (1, 1), (0, 0)), mode="constant"), earlier, speed_square)
        earlier, field_now = field_now, later
    return field_now
```

```python
import functools

import jax
import jax.numpy as jnp
from jax import lax
from jax.experimental import pallas as pl
from jax.experimental.pallas import tpu as pltpu
from jax.sharding import PartitionSpec as P

STEPS = 4
ROWS = 8
AXES = ("lat", "lon", "lev")


def kernel(peers, field, earlier, speed, out, even, odd, squares, lat_halo, lev_halo, lev_edge,
           lat_sent, lat_come, lon_sent, lon_come, lev_sent, lev_come, loaded, stored):
    J, I, K, M = field.shape
    rows = ROWS if I % ROWS == 0 else 1
    chunks = I // rows
    bufs = (even, odd)
    at = {axis: lax.axis_index(axis) for axis in AXES}
    has = {axis: (at[axis] > 0, at[axis] < peers[axis] - 1) for axis in AXES}
    ids = {axis: (lax.rem(at[axis] + peers[axis] - 1, peers[axis]), lax.rem(at[axis] + 1, peers[axis])) for axis in AXES}

    def remote(axis, side, src, dst, sent, come):
        return pltpu.make_async_remote_copy(
            src_ref=src, dst_ref=dst, send_sem=sent, recv_sem=come,
            device_id={axis: ids[axis][side]}, device_id_type=pl.DeviceIdType.MESH)

    def lat_copy(step, side, c):
        j = (J - 1) * side
        here = pl.ds(c * rows, rows)
        src = field.at[j, here] if step == 0 else bufs[step % 2].at[j, pl.ds(c * rows + 1, rows)]
        return remote("lat", side, src, lat_halo.at[step, 1 - side, here],
                      lat_sent.at[step, side, c], lat_come.at[step, 1 - side, c])

    def lon_copy(step, side):
        src = field.at[:, (I - 1) * side] if step == 0 else bufs[step % 2].at[:, 1 + (I - 1) * side]
        return remote("lon", side, src, bufs[step % 2].at[:, (I + 1) * (1 - side)],
                      lon_sent.at[step, side], lon_come.at[step, 1 - side])

    def lev_copy(step, side):
        return remote("lev", side, lev_edge.at[step, side], lev_halo.at[step, 1 - side],
                      lev_sent.at[step, side], lev_come.at[step, 1 - side])

    def each_side(axis, act):
        for side in (0, 1):
            pl.when(has[axis][side])(functools.partial(act, side))

    def load(which, c):
        src, dst, first = ((field, even, 1), (earlier, odd, 1), (speed, squares, 0))[which]
        return pltpu.make_async_copy(src.at[:, pl.ds(c * rows, rows)],
                                     dst.at[:, pl.ds(c * rows + first, rows)], loaded.at[which, c])

    def store(c):
        return pltpu.make_async_copy(bufs[STEPS % 2].at[:, pl.ds(c * rows + 1, rows)],
                                     out.at[:, pl.ds(c * rows, rows)], stored.at[c])

    def loop(count, body):
        lax.fori_loop(0, count, lambda n, carry: (body(n), carry)[1], 0)

    barrier = pltpu.get_barrier_semaphore()
    for axis in AXES:
        each_side(axis, lambda side: pl.semaphore_signal(
            barrier, inc=1, device_id={axis: ids[axis][side]}, device_id_type=pl.DeviceIdType.MESH))
    for which in range(3):
        loop(chunks, lambda c: load(which, c).start())
    pl.semaphore_wait(barrier, sum(there.astype(jnp.int32) for axis in AXES for there in has[axis]))

    @functools.partial(loop, chunks)
    def _(c):
        each_side("lat", lambda side: lat_copy(0, side, c).start())

    each_side("lon", lambda side: lon_copy(0, side).start())

    for side in (0, 1):
        @pl.when(jnp.logical_not(has["lat"][side]))
        def _():
            @functools.partial(loop, I)
            def _(i):
                for step in range(STEPS):
                    lat_halo[step, side, i] = jnp.zeros((K, M), jnp.float32)

        @pl.when(jnp.logical_not(has["lon"][side]))
        def _():
            for buf in bufs:
                for j in range(J):
                    buf[j, (I + 1) * side] = jnp.zeros((K, M), jnp.float32)

        @pl.when(jnp.logical_not(has["lev"][side]))
        def _():
            for step in range(STEPS):
                for j in range(J):
                    lev_halo[step, side, j] = jnp.zeros((I, M), jnp.float32)

    loop(chunks, lambda c: load(0, c).wait())

    @functools.partial(loop, I)
    def _(i):
        for j in range(J):
            for side in (0, 1):
                lev_edge[0, side, j, pl.ds(i, 1), :] = even[j, i + 1, pl.ds((K - 1) * side, 1), :]

    each_side("lev", lambda side: lev_copy(0, side).start())

    level = lax.broadcasted_iota(jnp.int32, (K, M), 0)
    for step in range(STEPS):
        now, then = bufs[step % 2], bufs[(step + 1) % 2]

        def row(i):
            for j in range(J):
                middle = now[j, i + 1]
                below = lat_halo[step, 0, i] if j == 0 else now[j - 1, i + 1]
                above = lat_halo[step, 1, i] if j == J - 1 else now[j + 1, i + 1]
                under = jnp.where(level == 0, lev_halo[step, 0, j, pl.ds(i, 1), :], pltpu.roll(middle, 1, 0))
                over = jnp.where(level == K - 1, lev_halo[step, 1, j, pl.ds(i, 1), :], pltpu.roll(middle, K - 1, 0))
                spread = below + above + now[j, i] + now[j, i + 2] + under + over - 6.0 * middle
                later = 2.0 * middle - then[j, i + 1] + squares[j, i] * spread
                then[j, i + 1] = later
                if step + 1 < STEPS:
                    lev_edge[step + 1, 0, j, pl.ds(i, 1), :] = later[:1]
                    lev_edge[step + 1, 1, j, pl.ds(i, 1), :] = later[K - 1:]

        for axis, copy in (("lon", lon_copy), ("lev", lev_copy)):
            if step > 0:
                each_side(axis, lambda side: copy(step - 1, side).wait_send())
            each_side(axis, lambda side: copy(step, 1 - side).wait_recv())

        @functools.partial(loop, chunks)
        def _(c):
            if step == 0:
                load(1, c).wait()
                load(2, c).wait()
            else:
                each_side("lat", lambda side: lat_copy(step - 1, side, c).wait_send())
            each_side("lat", lambda side: lat_copy(step, 1 - side, c).wait_recv())
            loop(rows, lambda r: row(c * rows + r))
            if step + 1 < STEPS:
                each_side("lat", lambda side: lat_copy(step + 1, side, c).start())
            else:
                store(c).start()

        if step + 1 < STEPS:
            each_side("lon", lambda side: lon_copy(step + 1, side).start())
            each_side("lev", lambda side: lev_copy(step + 1, side).start())

    for axis, copy in (("lon", lon_copy), ("lev", lev_copy)):
        each_side(axis, lambda side: copy(STEPS - 1, side).wait_send())

    @functools.partial(loop, chunks)
    def _(c):
        each_side("lat", lambda side: lat_copy(STEPS - 1, side, c).wait_send())
        store(c).wait()


def solution(mesh):
    peers = {axis: mesh.shape[axis] for axis in AXES}

    def local(field_now, earlier, speed_square):
        J, I, K, M = field_now.shape
        chunks = I // ROWS if I % ROWS == 0 else I
        dma = pltpu.SemaphoreType.DMA
        return pl.pallas_call(
            functools.partial(kernel, peers),
            out_shape=jax.ShapeDtypeStruct(field_now.shape, jnp.float32),
            in_specs=[pl.BlockSpec(memory_space=pltpu.HBM)] * 3,
            out_specs=pl.BlockSpec(memory_space=pltpu.HBM),
            scratch_shapes=[
                pltpu.VMEM((J, I + 2, K, M), jnp.float32),
                pltpu.VMEM((J, I + 2, K, M), jnp.float32),
                pltpu.VMEM((J, I, K, M), jnp.float32),
                pltpu.VMEM((STEPS, 2, I, K, M), jnp.float32),
                pltpu.VMEM((STEPS, 2, J, I, M), jnp.float32),
                pltpu.VMEM((STEPS, 2, J, I, M), jnp.float32),
                dma((STEPS, 2, chunks)), dma((STEPS, 2, chunks)),
                dma((STEPS, 2)), dma((STEPS, 2)),
                dma((STEPS, 2)), dma((STEPS, 2)),
                dma((3, chunks)), dma((chunks,)),
            ],
            compiler_params=pltpu.CompilerParams(
                collective_id=0, has_side_effects=True, vmem_limit_bytes=60 * 1024 * 1024),
        )(field_now, earlier, speed_square)

    spec = P("lat", "lon", "lev", None)
    return jax.shard_map(local, mesh=mesh, in_specs=(spec, spec, spec), out_specs=spec, check_vma=False)
```

```python
import functools

import jax
import jax.numpy as jnp
from jax import lax
from jax.experimental import pallas as pl
from jax.experimental.pallas import tpu as pltpu
from jax.sharding import PartitionSpec as P

STEPS = 4
AXES = ("lat", "lon", "lev")


def pieces(I):
    unit = I // 16
    table = [[4, 4, 4, 4]] * (STEPS - 1) + [[4, 4, 4, 2, 1, 1]]
    if I % 16:
        unit, table = I, [[1]] * STEPS
    return [[(unit * sum(sizes[:n]), unit * size) for n, size in enumerate(sizes)] for sizes in table]


def kernel(peers, field, earlier, speed, out, even, odd, squares, lat_halo, lev_halo, lev_edge,
           lat_sent, lat_come, lon_sent, lon_come, lev_sent, lev_come, loaded):
    J, I, K, M = field.shape
    parts = pieces(I)
    bufs = (even, odd)
    at = {axis: lax.axis_index(axis) for axis in AXES}
    has = {axis: (at[axis] > 0, at[axis] < peers[axis] - 1) for axis in AXES}
    ids = {axis: (lax.rem(at[axis] + peers[axis] - 1, peers[axis]), lax.rem(at[axis] + 1, peers[axis])) for axis in AXES}

    def remote(axis, side, src, dst, sent, come):
        return pltpu.make_async_remote_copy(
            src_ref=src, dst_ref=dst, send_sem=sent, recv_sem=come,
            device_id={axis: ids[axis][side]}, device_id_type=pl.DeviceIdType.MESH)

    def lat_copy(step, side, c):
        j = (J - 1) * side
        first, rows = parts[step][c]
        here = pl.ds(first, rows)
        src = field.at[j, here] if step == 0 else bufs[step % 2].at[j, pl.ds(first + 1, rows)]
        return remote("lat", side, src, lat_halo.at[step, 1 - side, here],
                      lat_sent.at[step, side, c], lat_come.at[step, 1 - side, c])

    def lon_copy(step, side):
        src = field.at[:, (I - 1) * side] if step == 0 else bufs[step % 2].at[:, 1 + (I - 1) * side]
        return remote("lon", side, src, bufs[step % 2].at[:, (I + 1) * (1 - side)],
                      lon_sent.at[step, side], lon_come.at[step, 1 - side])

    def lev_copy(step, side):
        return remote("lev", side, lev_edge.at[step, side], lev_halo.at[step, 1 - side],
                      lev_sent.at[step, side], lev_come.at[step, 1 - side])

    def each_side(axis, act):
        for side in (0, 1):
            pl.when(has[axis][side])(functools.partial(act, side))

    def load(which, c):
        src, dst, margin = ((field, even, 1), (earlier, odd, 1), (speed, squares, 0))[which]
        first, rows = parts[0][c]
        return pltpu.make_async_copy(src.at[:, pl.ds(first, rows)],
                                     dst.at[:, pl.ds(first + margin, rows)], loaded.at[which, c])

    def loop(count, body):
        lax.fori_loop(0, count, lambda n, carry: (body(n), carry)[1], 0)

    barrier = pltpu.get_barrier_semaphore()
    for axis in AXES:
        each_side(axis, lambda side: pl.semaphore_signal(
            barrier, inc=1, device_id={axis: ids[axis][side]}, device_id_type=pl.DeviceIdType.MESH))
    for which in range(3):
        for c in range(len(parts[0])):
            load(which, c).start()
    pl.semaphore_wait(barrier, sum(there.astype(jnp.int32) for axis in AXES for there in has[axis]))

    for c in range(len(parts[0])):
        each_side("lat", lambda side: lat_copy(0, side, c).start())

    each_side("lon", lambda side: lon_copy(0, side).start())

    for side in (0, 1):
        @pl.when(jnp.logical_not(has["lat"][side]))
        def _():
            @functools.partial(loop, I)
            def _(i):
                for step in range(STEPS):
                    lat_halo[step, side, i] = jnp.zeros((K, M), jnp.float32)

        @pl.when(jnp.logical_not(has["lon"][side]))
        def _():
            for buf in bufs:
                for j in range(J):
                    buf[j, (I + 1) * side] = jnp.zeros((K, M), jnp.float32)

        @pl.when(jnp.logical_not(has["lev"][side]))
        def _():
            for step in range(STEPS):
                for j in range(J):
                    lev_halo[step, side, j] = jnp.zeros((I, M), jnp.float32)

    for c in range(len(parts[0])):
        load(0, c).wait()

    @functools.partial(loop, I)
    def _(i):
        for j in range(J):
            for side in (0, 1):
                lev_edge[0, side, j, pl.ds(i, 1), :] = even[j, i + 1, pl.ds((K - 1) * side, 1), :]

    each_side("lev", lambda side: lev_copy(0, side).start())

    level = lax.broadcasted_iota(jnp.int32, (K, M), 0)
    for step in range(STEPS):
        now, then = bufs[step % 2], bufs[(step + 1) % 2]

        def row(i, planes):
            for j in planes:
                middle = now[j, i + 1]
                below = lat_halo[step, 0, i] if j == 0 else now[j - 1, i + 1]
                above = lat_halo[step, 1, i] if j == J - 1 else now[j + 1, i + 1]
                under = jnp.where(level == 0, lev_halo[step, 0, j, pl.ds(i, 1), :], pltpu.roll(middle, 1, 0))
                over = jnp.where(level == K - 1, lev_halo[step, 1, j, pl.ds(i, 1), :], pltpu.roll(middle, K - 1, 0))
                spread = below + above + now[j, i] + now[j, i + 2] + under + over - 6.0 * middle
                later = 2.0 * middle - then[j, i + 1] + squares[j, i] * spread
                if step + 1 == STEPS:
                    out[j, i] = later
                else:
                    then[j, i + 1] = later
                    lev_edge[step + 1, 0, j, pl.ds(i, 1), :] = later[:1]
                    lev_edge[step + 1, 1, j, pl.ds(i, 1), :] = later[K - 1:]

        for axis, copy in (("lon", lon_copy), ("lev", lev_copy)):
            if step > 0:
                each_side(axis, lambda side: copy(step - 1, side).wait_send())
            each_side(axis, lambda side: copy(step, 1 - side).wait_recv())

        if step + 1 == STEPS:
            for c in range(len(parts[step - 1])):
                each_side("lat", lambda side: lat_copy(step - 1, side, c).wait_send())
            loop(I, lambda i: row(i, range(1, J - 1)))
        for c, (first, rows) in enumerate(parts[step]):
            if step == 0:
                load(1, c).wait()
                load(2, c).wait()
            elif step + 1 < STEPS:
                each_side("lat", lambda side: lat_copy(step - 1, side, c).wait_send())
            each_side("lat", lambda side: lat_copy(step, 1 - side, c).wait_recv())
            planes = (0, J - 1)[: min(J, 2)] if step + 1 == STEPS else range(J)
            loop(rows, lambda r: row(first + r, planes))
            if step + 1 < STEPS:
                for d, (start, size) in enumerate(parts[step + 1]):
                    if first < start + size <= first + rows:
                        each_side("lat", lambda side: lat_copy(step + 1, side, d).start())

        if step + 1 < STEPS:
            each_side("lon", lambda side: lon_copy(step + 1, side).start())
            each_side("lev", lambda side: lev_copy(step + 1, side).start())

    for axis, copy in (("lon", lon_copy), ("lev", lev_copy)):
        each_side(axis, lambda side: copy(STEPS - 1, side).wait_send())

    for c in range(len(parts[-1])):
        each_side("lat", lambda side: lat_copy(STEPS - 1, side, c).wait_send())


def solution(mesh):
    peers = {axis: mesh.shape[axis] for axis in AXES}

    def local(field_now, earlier, speed_square):
        J, I, K, M = field_now.shape
        chunks = max(len(part) for part in pieces(I))
        dma = pltpu.SemaphoreType.DMA
        return pl.pallas_call(
            functools.partial(kernel, peers),
            out_shape=pltpu.VMEM(field_now.shape, jnp.float32),
            in_specs=[pl.BlockSpec(memory_space=pltpu.HBM)] * 3,
            out_specs=pl.BlockSpec(memory_space=pltpu.VMEM),
            scratch_shapes=[
                pltpu.VMEM((J, I + 2, K, M), jnp.float32),
                pltpu.VMEM((J, I + 2, K, M), jnp.float32),
                pltpu.VMEM((J, I, K, M), jnp.float32),
                pltpu.VMEM((STEPS, 2, I, K, M), jnp.float32),
                pltpu.VMEM((STEPS, 2, J, I, M), jnp.float32),
                pltpu.VMEM((STEPS, 2, J, I, M), jnp.float32),
                dma((STEPS, 2, chunks)), dma((STEPS, 2, chunks)),
                dma((STEPS, 2)), dma((STEPS, 2)),
                dma((STEPS, 2)), dma((STEPS, 2)),
                dma((3, chunks)),
            ],
            compiler_params=pltpu.CompilerParams(
                collective_id=0, has_side_effects=True, vmem_limit_bytes=48000 * 1024),
        )(field_now, earlier, speed_square)

    spec = P("lat", "lon", "lev", None)
    return jax.shard_map(local, mesh=mesh, in_specs=(spec, spec, spec), out_specs=spec, check_vma=False)
```

```python
import functools

import jax
import jax.numpy as jnp
from jax import lax
from jax.experimental import pallas as pl
from jax.experimental.pallas import tpu as pltpu
from jax.sharding import PartitionSpec as P

STEPS = 4
AXES = ("lat", "lon", "lev")


def pieces(I):
    unit = I // 16
    table = [[8, 4, 4]] * (STEPS - 1) + [[8, 4, 2, 2]]
    if I % 16:
        unit, table = I, [[1]] * STEPS
    return [[(unit * sum(sizes[:n]), unit * size) for n, size in enumerate(sizes)] for sizes in table]


def kernel(peers, field, earlier, speed, out, even, odd, squares, lat_halo, lev_halo, lev_edge,
           lat_sent, lat_come, lon_sent, lon_come, lev_sent, lev_come, loaded):
    J, I, K, M = field.shape
    parts = pieces(I)
    bufs = (even, odd)
    at = {axis: lax.axis_index(axis) for axis in AXES}
    has = {axis: (at[axis] > 0, at[axis] < peers[axis] - 1) for axis in AXES}
    ids = {axis: (lax.rem(at[axis] + peers[axis] - 1, peers[axis]), lax.rem(at[axis] + 1, peers[axis])) for axis in AXES}

    def remote(axis, side, src, dst, sent, come):
        return pltpu.make_async_remote_copy(
            src_ref=src, dst_ref=dst, send_sem=sent, recv_sem=come,
            device_id={axis: ids[axis][side]}, device_id_type=pl.DeviceIdType.MESH)

    def lat_copy(step, side, c):
        j = (J - 1) * side
        first, rows = parts[step][c]
        here = pl.ds(first, rows)
        src = field.at[j, here] if step == 0 else bufs[step % 2].at[j, pl.ds(first + 1, rows)]
        return remote("lat", side, src, lat_halo.at[step, 1 - side, here],
                      lat_sent.at[step, side, c], lat_come.at[step, 1 - side, c])

    def lon_copy(step, side):
        src = field.at[:, (I - 1) * side] if step == 0 else bufs[step % 2].at[:, 1 + (I - 1) * side]
        return remote("lon", side, src, bufs[step % 2].at[:, (I + 1) * (1 - side)],
                      lon_sent.at[step, side], lon_come.at[step, 1 - side])

    def lev_copy(step, side):
        return remote("lev", side, lev_edge.at[step, side], lev_halo.at[step, 1 - side],
                      lev_sent.at[step, side], lev_come.at[step, 1 - side])

    def each_side(axis, act):
        for side in (0, 1):
            pl.when(has[axis][side])(functools.partial(act, side))

    def load(which, c):
        src, dst, margin = ((field, even, 1), (earlier, odd, 1), (speed, squares, 0))[which]
        first, rows = parts[0][c]
        return pltpu.make_async_copy(src.at[:, pl.ds(first, rows)],
                                     dst.at[:, pl.ds(first + margin, rows)], loaded.at[which, c])

    def loop(count, body):
        lax.fori_loop(0, count, lambda n, carry: (body(n), carry)[1], 0)

    barrier = pltpu.get_barrier_semaphore()
    for axis in AXES:
        each_side(axis, lambda side: pl.semaphore_signal(
            barrier, inc=1, device_id={axis: ids[axis][side]}, device_id_type=pl.DeviceIdType.MESH))
    for which in range(3):
        for c in range(len(parts[0])):
            load(which, c).start()
    pl.semaphore_wait(barrier, sum(there.astype(jnp.int32) for axis in AXES for there in has[axis]))

    for c in range(len(parts[0])):
        each_side("lat", lambda side: lat_copy(0, side, c).start())

    each_side("lon", lambda side: lon_copy(0, side).start())

    for side in (0, 1):
        @pl.when(jnp.logical_not(has["lat"][side]))
        def _():
            @functools.partial(loop, I)
            def _(i):
                for step in range(STEPS):
                    lat_halo[step, side, i] = jnp.zeros((K, M), jnp.float32)

        @pl.when(jnp.logical_not(has["lon"][side]))
        def _():
            for buf in bufs:
                for j in range(J):
                    buf[j, (I + 1) * side] = jnp.zeros((K, M), jnp.float32)

        @pl.when(jnp.logical_not(has["lev"][side]))
        def _():
            for step in range(STEPS):
                for j in range(J):
                    lev_halo[step, side, j] = jnp.zeros((I, M), jnp.float32)

    for c in range(len(parts[0])):
        load(0, c).wait()

    @functools.partial(loop, I)
    def _(i):
        for j in range(J):
            for side in (0, 1):
                lev_edge[0, side, j, pl.ds(i, 1), :] = even[j, i + 1, pl.ds((K - 1) * side, 1), :]

    each_side("lev", lambda side: lev_copy(0, side).start())

    level = lax.broadcasted_iota(jnp.int32, (K, M), 0)
    for step in range(STEPS):
        now, then = bufs[step % 2], bufs[(step + 1) % 2]

        def row(i, planes):
            for j in planes:
                middle = now[j, i + 1]
                below = lat_halo[step, 0, i] if j == 0 else now[j - 1, i + 1]
                above = lat_halo[step, 1, i] if j == J - 1 else now[j + 1, i + 1]
                under = jnp.where(level == 0, lev_halo[step, 0, j, pl.ds(i, 1), :], pltpu.roll(middle, 1, 0))
                over = jnp.where(level == K - 1, lev_halo[step, 1, j, pl.ds(i, 1), :], pltpu.roll(middle, K - 1, 0))
                spread = below + above + now[j, i] + now[j, i + 2] + under + over - 6.0 * middle
                later = 2.0 * middle - then[j, i + 1] + squares[j, i] * spread
                if step + 1 == STEPS:
                    out[j, i] = later
                else:
                    then[j, i + 1] = later
                    lev_edge[step + 1, 0, j, pl.ds(i, 1), :] = later[:1]
                    lev_edge[step + 1, 1, j, pl.ds(i, 1), :] = later[K - 1:]

        for axis, copy in (("lon", lon_copy), ("lev", lev_copy)):
            if step > 0:
                each_side(axis, lambda side: copy(step - 1, side).wait_send())
            each_side(axis, lambda side: copy(step, 1 - side).wait_recv())

        if step + 1 == STEPS:
            for c in range(len(parts[step - 1])):
                each_side("lat", lambda side: lat_copy(step - 1, side, c).wait_send())
            loop(I, lambda i: row(i, range(1, J - 1)))
        for c, (first, rows) in enumerate(parts[step]):
            if step == 0:
                load(1, c).wait()
                load(2, c).wait()
            elif step + 1 < STEPS:
                each_side("lat", lambda side: lat_copy(step - 1, side, c).wait_send())
            each_side("lat", lambda side: lat_copy(step, 1 - side, c).wait_recv())
            planes = (0, J - 1)[: min(J, 2)] if step + 1 == STEPS else range(J)
            loop(rows, lambda r: row(first + r, planes))
            if step + 1 < STEPS:
                for d, (start, size) in enumerate(parts[step + 1]):
                    if first < start + size <= first + rows:
                        each_side("lat", lambda side: lat_copy(step + 1, side, d).start())

        if step + 1 < STEPS:
            each_side("lon", lambda side: lon_copy(step + 1, side).start())
            each_side("lev", lambda side: lev_copy(step + 1, side).start())

    for axis, copy in (("lon", lon_copy), ("lev", lev_copy)):
        each_side(axis, lambda side: copy(STEPS - 1, side).wait_send())

    for c in range(len(parts[-1])):
        each_side("lat", lambda side: lat_copy(STEPS - 1, side, c).wait_send())


def solution(mesh):
    peers = {axis: mesh.shape[axis] for axis in AXES}

    def local(field_now, earlier, speed_square):
        J, I, K, M = field_now.shape
        chunks = max(len(part) for part in pieces(I))
        dma = pltpu.SemaphoreType.DMA
        return pl.pallas_call(
            functools.partial(kernel, peers),
            out_shape=pltpu.VMEM(field_now.shape, jnp.float32),
            in_specs=[pl.BlockSpec(memory_space=pltpu.HBM)] * 3,
            out_specs=pl.BlockSpec(memory_space=pltpu.VMEM),
            scratch_shapes=[
                pltpu.VMEM((J, I + 2, K, M), jnp.float32),
                pltpu.VMEM((J, I + 2, K, M), jnp.float32),
                pltpu.VMEM((J, I, K, M), jnp.float32),
                pltpu.VMEM((STEPS, 2, I, K, M), jnp.float32),
                pltpu.VMEM((STEPS, 2, J, I, M), jnp.float32),
                pltpu.VMEM((STEPS, 2, J, I, M), jnp.float32),
                dma((STEPS, 2, chunks)), dma((STEPS, 2, chunks)),
                dma((STEPS, 2)), dma((STEPS, 2)),
                dma((STEPS, 2)), dma((STEPS, 2)),
                dma((3, chunks)),
            ],
            compiler_params=pltpu.CompilerParams(
                collective_id=0, has_side_effects=True, vmem_limit_bytes=48000 * 1024),
        )(field_now, earlier, speed_square)

    spec = P("lat", "lon", "lev", None)
    return jax.shard_map(local, mesh=mesh, in_specs=(spec, spec, spec), out_specs=spec, check_vma=False)
```
